128 devices in a mesh: res: 32 (over x_lo, y, z), seq: 4 (over x_hi, core).
Axes of the slice: x: 4 (x_hi: 2, x_lo: 2; x = x_hi * 2 + x_lo), y: 4, z: 4, core: 2. Of those that a mesh axis runs over, the one named last changes fastest.
Arguments:
- alignment: bfloat16 [384, 1024, 256], P('seq', 'res'), may hold values from -6 to 6
- query_weight: bfloat16 [256, 256], replicated, may hold values from -1 to 1
- w_keyval: bfloat16 [256, 512], replicated, may hold values from -0.375 to 0.375
- w_gate: bfloat16 [256, 256], replicated, may hold values from -0.375 to 0.375
- output_weight: bfloat16 [256, 256], replicated, may hold values from -0.75 to 0.75
- w_factors: bfloat16 [256, 64], replicated, may hold values from -1.5 to 1.5
- w_pair_out: bfloat16 [1024, 128], replicated, may hold values from -0.1875 to 0.1875
Outputs:
- alignment_update: bfloat16 [384, 1024, 256], P('seq', 'res')
- pair_representation_update: bfloat16 [1024, 1024, 128], P(('res', 'seq'))
The draws below stay inside these ranges and needn't reach their ends.
All inputs are finite; a program needn't handle non-finite values.
Results may differ from the reference program's by a relative error of at most 0.012.
The reference program's roundings to bfloat16 on the way count: a program that leaves them out, or rounds other values in their place, can miss the bound.
Values may be sent and summed in bfloat16 or wider, within the bound.
No kernel may reach another device: no remote copies, remote signals or barrier semaphores. Data moves between devices by JAX's collectives and lax.ppermute only.
A program may use at most 256 MiB of HBM per device.

```python
import math
import jax
import jax.numpy as jnp
from jax import lax

D = 256
P_SIZE = 128
HEADS = 8
HC = 32
C = 32
HD = 256
S = 384
R = 1024


def levels(own_key, dims, pieces, low, largest):
    gain, own = 1.0, jax.random.fold_in(own_key, 6)
    for position, shards_of in pieces:
        draws = jnp.exp(jax.random.uniform(jax.random.fold_in(own, position), (shards_of,), jnp.float32, low / len(pieces), largest / len(pieces)))
        gain = gain * jnp.repeat(draws, dims[position] // shards_of).reshape([-1 if axis == position else 1 for axis in range(len(dims))])
    return gain


def bell_draw(rng, shape, deviation, bound, pieces=(), held_as=jnp.bfloat16):
    drawn = deviation * jax.random.normal(rng, shape, jnp.float32)
    if pieces:
        drawn = drawn * levels(rng, shape, pieces, -0.22, 0.18)
    return jnp.clip(drawn, -bound, bound).astype(held_as)


def setup_inputs(seed: int = 0) -> dict:
    key_list = jax.random.split(jax.random.key(seed), 8)
    return {
        "alignment": bell_draw(key_list[0], (S, R, D), 1.0, 6.0, ((0, 4), (1, 32))),
        "query_weight": bell_draw(key_list[1], (D, HD), (D // 9) ** -0.5, 1.0),
        "w_keyval": bell_draw(key_list[2], (D, 2 * HD), D ** -0.5, 0.375),
        "w_gate": bell_draw(key_list[3], (D, HD), D ** -0.5, 0.375),
        "output_weight": bell_draw(key_list[4], (HD, D), (HD // 4) ** -0.5, 0.75),
        "w_factors": bell_draw(key_list[5], (D, 2 * C), (D // 16) ** -0.5, 1.5),
        "w_pair_out": bell_draw(key_list[6], (C * C, P_SIZE), (C * C) ** -0.5, 0.1875),
    }


def normalize(alignment):
    values = alignment.astype(jnp.float32)
    centered = values - lax.optimization_barrier(jnp.mean(values, axis=-1, keepdims=True))
    spread = lax.optimization_barrier(jnp.mean(centered * centered, axis=-1, keepdims=True))
    return (centered * lax.rsqrt(spread + 1e-05)).astype(jnp.bfloat16)

def reference(alignment, query_weight, w_keyval, w_gate, output_weight, w_factors, w_pair_out):
    normed = normalize(alignment)
    queries = jnp.dot(normed, query_weight, preferred_element_type=jnp.float32).astype(jnp.bfloat16)
    keyvals = jnp.dot(normed, w_keyval, preferred_element_type=jnp.float32).astype(jnp.bfloat16)
    gating = jax.nn.sigmoid(jnp.dot(normed, w_gate, preferred_element_type=jnp.float32))
    hidden = HEADS * HC
    seq_total = normed.shape[0]
    residues = normed.shape[1]
    group_size = math.gcd(residues, 8)

    def attend_block(block_index):
        start_row = (block_index * group_size).astype(jnp.int32)
        query_block = lax.dynamic_slice_in_dim(queries, start_row, group_size, 1).astype(jnp.float32)
        keyval_block = lax.dynamic_slice_in_dim(keyvals, start_row, group_size, 1).astype(jnp.float32)
        per_head_query = query_block.reshape(seq_total, group_size, HEADS, HC)
        head_keys = keyval_block[:, :, :hidden].reshape(seq_total, group_size, HEADS, HC)
        head_values = keyval_block[:, :, hidden:].reshape(seq_total, group_size, HEADS, HC)
        scores = jnp.einsum('qrhd,krhd->rhqk', per_head_query, head_keys) / math.sqrt(HC)
        exponent = jnp.exp(scores)
        weights = exponent.astype(jnp.bfloat16).astype(jnp.float32)
        denominators = jnp.transpose(lax.optimization_barrier(jnp.sum(exponent, axis=-1)), (2, 0, 1))
        weighted = jnp.einsum('rhqk,krhd->qrhd', weights, head_values)
        return (weighted / denominators[:, :, :, None]).reshape(seq_total, group_size, hidden)
    blocks = lax.map(attend_block, jnp.arange(residues // group_size, dtype=jnp.int32))
    attended = jnp.transpose(blocks, (1, 0, 2, 3)).reshape(seq_total, residues, hidden)
    gated_output_rows = (gating * attended).astype(jnp.bfloat16)
    alignment_update = jnp.dot(gated_output_rows, output_weight, preferred_element_type=jnp.float32).astype(jnp.bfloat16)
    factors = jnp.dot(normed, w_factors, preferred_element_type=jnp.float32).astype(jnp.bfloat16)
    factor = factors.shape[2] // 2
    left_factor = factors[:, :, :factor].astype(jnp.float32).reshape(seq_total, residues * factor)
    right_factor = factors[:, :, factor:].astype(jnp.float32).reshape(seq_total, residues * factor)
    channels = w_pair_out.shape[1]
    pair_weight = w_pair_out.astype(jnp.float32).reshape(factor, factor, channels)
    row_block = math.gcd(residues, 32)

    def pair_block(block_index):
        start_col = (block_index * row_block * factor).astype(jnp.int32)
        left_rows = lax.dynamic_slice_in_dim(left_factor, start_col, row_block * factor, 1)
        products = lax.dot_general(left_rows, right_factor, (((0,), (0,)), ((), ())), precision=lax.Precision.HIGHEST, preferred_element_type=jnp.float32)
        products = (products * (1.0 / seq_total)).reshape(row_block, factor, residues, factor)
        return jnp.einsum('icje,cep->ijp', products, pair_weight, precision=lax.Precision.HIGHEST)
    pair_blocks = lax.map(pair_block, jnp.arange(residues // row_block, dtype=jnp.int32))
    pair_representation_update = pair_blocks.reshape(residues, residues, channels).astype(jnp.bfloat16)
    return (alignment_update, pair_representation_update)
```

```python
import math

import jax
import jax.numpy as jnp
from jax import lax
from jax.experimental import pallas as pl
from jax.experimental.pallas import tpu as pltpu
from jax.sharding import Mesh
from jax.sharding import PartitionSpec as P

HEADS = 8
HC = 32
EPS = 1e-05
SEQ = ("xh", "c")
ROWS = ("yl", "z")
COLS = ("xl", "yh", "xh", "c")
NT = (((1,), (1,)), ((), ()))
NN = (((1,), (0,)), ((), ()))
TN = (((0,), (0,)), ((), ()))
F32 = jnp.float32
BF16 = jnp.bfloat16


def dot(a, b, dims):
    return lax.dot_general(a, b, dims, preferred_element_type=F32)


def norm_kernel(x_ref, wf_ref, n_ref, l_ref, r_ref, nf, rf):
    rows = x_ref.shape[0]
    step = 256

    def one(k, _):
        sl = pl.ds(pl.multiple_of(k * step, step), step)
        v = x_ref[sl, :].astype(F32)
        v = v - jnp.mean(v, axis=-1, keepdims=True)
        spread = jnp.mean(v * v, axis=-1, keepdims=True)
        y = (v * lax.rsqrt(spread + EPS)).astype(BF16).astype(F32)
        nf[0, sl, :] = y[:, :128]
        nf[1, sl, :] = y[:, 128:]
        return 0

    lax.fori_loop(0, rows // step, one, 0)
    seqs = rows // 8
    for r in range(8):
        x = jnp.concatenate(
            [nf[0, pl.ds(r, seqs, stride=8), :], nf[1, pl.ds(r, seqs, stride=8), :]], axis=1
        ).astype(BF16)
        n_ref[r] = x
        f = dot(wf_ref[...], x, NT)
        l_ref[r] = f[:32].astype(BF16)
        for t in range(3):
            rf[t, pl.ds(r, 32, stride=8), :] = f[32:, t * 128:(t + 1) * 128]
    for t in range(3):
        r_ref[:, t * 128:(t + 1) * 128] = rf[t].astype(BF16)


def norm_and_factors(x, wf_t):
    rows = x.shape[0]
    seqs = rows // 8
    return pl.pallas_call(
        norm_kernel,
        out_shape=(
            jax.ShapeDtypeStruct((8, seqs, 256), BF16),
            jax.ShapeDtypeStruct((8, 32, seqs), BF16),
            jax.ShapeDtypeStruct((256, seqs), BF16),
        ),
        scratch_shapes=[pltpu.VMEM((2, rows, 128), F32), pltpu.VMEM((3, 256, 128), F32)],
        cost_estimate=pl.CostEstimate(flops=2 * rows * 256 * 64, transcendentals=rows, bytes_accessed=4 * rows * 256),
        name="norm_factors",
    )(x, wf_t)


def attention_kernel(x_ref, wq_ref, wk_ref, wv_ref, wg_ref, wo_ref, o_ref, of):
    r = pl.program_id(0)
    x = x_ref[0]
    seqs = x.shape[0]
    q_t = dot(wq_ref[...], x, NT).astype(BF16)
    keys = dot(x, wk_ref[...], NN).astype(BF16)
    v_t = dot(wv_ref[...], x, NT).astype(BF16)
    g_t = jax.nn.sigmoid(dot(wg_ref[...], x, NT))
    ones = jnp.ones((16, seqs), BF16)
    scale = math.log2(math.e) / math.sqrt(HC)
    gated = []

    def spread(h):
        parts = []
        if h:
            parts.append(jnp.zeros((h * HC, seqs), BF16))
        parts.append(q_t[h * HC:(h + 1) * HC])
        if h < HEADS - 1:
            parts.append(jnp.zeros(((HEADS - 1 - h) * HC, seqs), BF16))
        return jnp.concatenate(parts, axis=0)

    for p in range(HEADS // 2):
        rhs = jnp.concatenate([spread(2 * p), spread(2 * p + 1)], axis=1)
        scores = dot(keys, rhs, NN)
        weights = jnp.exp2(scores * scale).astype(BF16)
        for u in range(2):
            h = 2 * p + u
            lhs = jnp.concatenate([v_t[h * HC:(h + 1) * HC], ones], axis=0)
            out = dot(lhs, weights[:, u * seqs:(u + 1) * seqs], NN)
            att = out[:HC] / out[HC:HC + 1]
            gated.append((g_t[h * HC:(h + 1) * HC] * att).astype(BF16))
    gated = jnp.concatenate(gated, axis=0)
    update = dot(gated, wo_ref[...], TN)
    of[0, pl.ds(r, seqs, stride=8), :] = update[:, :128]
    of[1, pl.ds(r, seqs, stride=8), :] = update[:, 128:]

    @pl.when(r == pl.num_programs(0) - 1)
    def _():
        o_ref[:, :128] = of[0].astype(BF16)
        o_ref[:, 128:] = of[1].astype(BF16)


def attention(normed, wq_t, wk, wv_t, wg_t, wo):
    count, seqs, width = normed.shape
    full = pl.BlockSpec((256, 256), lambda r: (0, 0))
    return pl.pallas_call(
        attention_kernel,
        grid=(count,),
        in_specs=[pl.BlockSpec((1, seqs, width), lambda r: (r, 0, 0)), full, full, full, full, full],
        out_specs=pl.BlockSpec((seqs * count, width), lambda r: (0, 0)),
        out_shape=jax.ShapeDtypeStruct((seqs * count, width), BF16),
        scratch_shapes=[pltpu.VMEM((2, seqs * count, 128), F32)],
        cost_estimate=pl.CostEstimate(
            flops=count * (2 * seqs * seqs * 256 * 9 + 2 * seqs * 256 * 256 * 5),
            transcendentals=count * HEADS * seqs * seqs,
            bytes_accessed=4 * count * seqs * width,
        ),
        name="attention",
    )(normed, wq_t, wk, wv_t, wg_t, wo)


def pair_kernel(scaling, l_ref, r_ref, w_ref, o_ref, scr):
    seqs = l_ref.shape[-1]
    left = l_ref[...].reshape(512, seqs)
    for n in range(8):
        right = r_ref[n * 512:(n + 1) * 512, :]
        o = dot(left, right, NT).astype(BF16)
        for i in range(16):
            for e in range(4):
                row = (n * 4 + e) * 32
                scr[i, row:row + 32, :] = o[i * 32:(i + 1) * 32, e * 128:(e + 1) * 128]
    for k in range(8):
        rhs = jnp.concatenate([scr[2 * k], scr[2 * k + 1]], axis=1)
        t = dot(w_ref[...], rhs, NN) * scaling
        o_ref[k, 0] = t[:, :128].T.astype(BF16)
        o_ref[k, 1] = t[:, 128:].T.astype(BF16)


def pair_block(left, right, w_t, part, scaling):
    seqs = left.shape[-1]
    return pl.pallas_call(
        lambda *refs: pair_kernel(scaling, *refs),
        grid=(1,),
        in_specs=[
            pl.BlockSpec((8, 2, 32, seqs), lambda g: (0, part, 0, 0)),
            pl.BlockSpec((4096, seqs), lambda g: (0, 0)),
            pl.BlockSpec((128, 1024), lambda g: (0, 0)),
        ],
        out_specs=pl.BlockSpec((8, 2, 128, 128), lambda g: (0, 0, 0, 0)),
        out_shape=jax.ShapeDtypeStruct((8, 2, 128, 128), BF16),
        scratch_shapes=[pltpu.VMEM((16, 1024, 128), BF16)],
        cost_estimate=pl.CostEstimate(
            flops=2 * 512 * 4096 * seqs + 2 * 16 * 128 * 128 * 1024,
            transcendentals=0,
            bytes_accessed=2 * (4096 + 512) * seqs,
        ),
        name="pair",
    )(left, right, w_t)


def spread_to(x, axes):
    n = lax.axis_size(axes)
    return lax.all_to_all(jnp.broadcast_to(x[None], (n, *x.shape)), axes, 0, 0)


def per_device(alignment, query_weight, w_keyval, w_gate, output_weight, w_factors, w_pair_out):
    seqs, residues, width = alignment.shape
    groups = 4
    own = residues // groups
    total = seqs * groups
    send = alignment.reshape(seqs, groups, own, width).transpose(1, 0, 2, 3)
    rows = lax.all_to_all(send, SEQ, 0, 0).reshape(total * own, width)
    normed, left, right = norm_and_factors(rows, w_factors.T)
    left_all = spread_to(left, ROWS)
    right_all = spread_to(right.reshape(32, 8, total), COLS)
    right_all = right_all.transpose(1, 0, 2, 3).reshape(32 * 128, total)
    update = attention(
        normed, query_weight.T, w_keyval[:, :256], w_keyval[:, 256:].T, w_gate.T, output_weight
    )
    back = lax.all_to_all(update.reshape(groups, seqs, own, width), SEQ, 0, 0)
    alignment_update = back.transpose(1, 0, 2, 3).reshape(seqs, residues, width)
    w_t = w_pair_out.reshape(32, 32, 128).transpose(2, 1, 0).reshape(128, 1024)
    pieces = []
    for part in range(4):
        block = pair_block(left_all, right_all, w_t, part, 1.0 / total)
        got = lax.all_to_all(block, ROWS, 0, 0)
        pieces.append(got.reshape(8, 2, 4, 32, 128).transpose(1, 2, 0, 3, 4).reshape(2, 1024, 128))
    return alignment_update, jnp.concatenate(pieces, axis=0)


def solution(mesh):
    split = Mesh(
        mesh.devices.reshape(2, 2, 2, 4, 2, 2), ("xl", "yh", "yl", "z", "xh", "c")
    )
    res = ("xl", "yh", "yl", "z")
    in_specs = (P(SEQ, res, None), P(), P(), P(), P(), P(), P())
    out_specs = (P(SEQ, res, None), P((*res, *SEQ), None, None))
    return jax.shard_map(
        per_device, mesh=split, in_specs=in_specs, out_specs=out_specs, check_vma=False
    )
```

```python
import math

import jax
import jax.numpy as jnp
from jax import lax
from jax.experimental import pallas as pl
from jax.experimental.pallas import tpu as pltpu
from jax.sharding import Mesh
from jax.sharding import PartitionSpec as P


HEADS = 8
HC = 32
EPS = 1e-05
SEQ = ("xh", "c")
ROWS = ("yl", "z")
XY = ("xl", "yh", "xh")
NT = (((1,), (1,)), ((), ()))
NN = (((1,), (0,)), ((), ()))
TN = (((0,), (0,)), ((), ()))
F32 = jnp.float32
BF16 = jnp.bfloat16


def dot(a, b, dims):
    return lax.dot_general(a, b, dims, preferred_element_type=F32)


def after(*arrays):
    return [pl.BlockSpec(memory_space=pl.ANY)] * len(arrays)


def front_kernel(q_ref, x_ref, wf_ref, n0, n1, n2, n3, l0, l1, l2, l3, r_ref, nf, nb, lf, rf, lb):
    rows = x_ref.shape[0]
    seqs = rows // 32
    step = 256

    def one(n, _):
        at = pl.ds(pl.multiple_of(n * step, step), step)
        v = x_ref[at, :].astype(F32)
        v = v - jnp.mean(v, axis=-1, keepdims=True)
        spread = jnp.mean(v * v, axis=-1, keepdims=True)
        y = v * lax.rsqrt(spread + EPS)
        nf[0, at, :] = y[:, :128]
        nf[1, at, :] = y[:, 128:]
        return 0

    lax.fori_loop(0, rows // step, one, 0)
    for r in range(32):
        at = pl.ds(r, seqs, stride=32)
        x = jnp.concatenate([nf[0, at, :], nf[1, at, :]], axis=1).astype(BF16)
        nb[r] = x
        f = dot(wf_ref[...], x, NT)
        lf[r * 32:(r + 1) * 32, :seqs] = f[:32]
        rf[pl.ds(r, 32, stride=32), :] = jnp.concatenate([f[32:], jnp.zeros((32, 128 - seqs), F32)], axis=1)
    for g in range(8):
        sl = slice(g * 128, (g + 1) * 128)
        r_ref[:, sl] = rf[sl, :].T[:seqs].astype(BF16)
        lb[g // 2, :, (g % 2) * 128:(g % 2 + 1) * 128] = lf[sl, :].T[:seqs].astype(BF16)
    q = q_ref[0]
    for k, (n_ref, l_ref) in enumerate(((n0, l0), (n1, l1), (n2, l2), (n3, l3))):
        for r in range(8):
            n_ref[r] = nb[(q ^ k) * 8 + r]
        l_ref[...] = lb[q ^ k]


def front(q, x, wf_t):
    rows = x.shape[0]
    seqs = rows // 32
    vmem = pl.BlockSpec(memory_space=pltpu.VMEM)
    outs = pl.pallas_call(
        front_kernel,
        in_specs=[pl.BlockSpec(memory_space=pltpu.SMEM), vmem, vmem],
        out_shape=[jax.ShapeDtypeStruct((8, seqs, 256), BF16)] * 4
        + [jax.ShapeDtypeStruct((seqs, 256), BF16)] * 4
        + [jax.ShapeDtypeStruct((seqs, 1024), BF16)],
        scratch_shapes=[
            pltpu.VMEM((2, rows, 128), F32),
            pltpu.VMEM((32, seqs, 256), BF16),
            pltpu.VMEM((1024, 128), F32),
            pltpu.VMEM((1024, 128), F32),
            pltpu.VMEM((4, seqs, 256), BF16),
        ],
        cost_estimate=pl.CostEstimate(flops=800_000_000, transcendentals=rows, bytes_accessed=4 * rows * 256),
        name="front",
    )(q, x, wf_t)
    return outs[:4], outs[4:8], outs[8]


def merge_left(pieces):
    seqs = pieces[0].shape[0] * 4

    def kernel(p0, p1, p2, p3, o_ref):
        x = jnp.concatenate([p0[...], p1[...], p2[...], p3[...]], axis=0).astype(F32)
        o_ref[...] = x.T.astype(BF16)

    vmem = pl.BlockSpec(memory_space=pltpu.VMEM)
    out = pl.pallas_call(
        kernel,
        in_specs=[vmem] * 4,
        out_shape=jax.ShapeDtypeStruct((256, seqs), BF16),
        cost_estimate=pl.CostEstimate(flops=100_000_000, transcendentals=0, bytes_accessed=4 * 256 * seqs),
        name="merge_left",
    )(*pieces)
    return out.reshape(8, 32, seqs)


def attention_kernel(which, n_wait, *refs):
    x_refs, (wq_ref, wk_ref, wv_ref, wg_ref, wo_ref) = refs[:4], refs[4:9]
    oa, ob, of = refs[9 + n_wait:]
    r = pl.program_id(0)
    part = x_refs[0].shape[1]
    x = jnp.concatenate([b[0] for b in x_refs], axis=0)
    mine = x[which * part:(which + 2) * part]
    seqs = 2 * part
    q_t = dot(wq_ref[...], mine, NT).astype(BF16)
    keys = dot(x, wk_ref[...], NN).astype(BF16)
    v_t = dot(wv_ref[...], x, NT).astype(BF16)
    g_t = jax.nn.sigmoid(dot(wg_ref[...], mine, NT))
    ones = jnp.ones((16, 4 * part), BF16)
    scale = math.log2(math.e) / math.sqrt(HC)
    gated = []

    def spread(h):
        parts = []
        if h:
            parts.append(jnp.zeros((h * HC, seqs), BF16))
        parts.append(q_t[h * HC:(h + 1) * HC])
        if h < HEADS - 1:
            parts.append(jnp.zeros(((HEADS - 1 - h) * HC, seqs), BF16))
        return jnp.concatenate(parts, axis=0)

    for p in range(HEADS // 4):
        rhs = jnp.concatenate([spread(4 * p + u) for u in range(4)], axis=1)
        scores = dot(keys, rhs, NN)
        weights = jnp.exp2(scores * scale).astype(BF16)
        for u in range(2):
            h = 4 * p + 2 * u
            lhs = jnp.concatenate([v_t[h * HC:(h + 2) * HC], ones], axis=0)
            out = dot(lhs, weights[:, u * 2 * seqs:(u + 1) * 2 * seqs], NN)
            inv = 1.0 / out[2 * HC:2 * HC + 1]
            for w in range(2):
                lanes = slice(w * seqs, (w + 1) * seqs)
                att = out[w * HC:(w + 1) * HC, lanes] * inv[:, lanes]
                gated.append((g_t[(h + w) * HC:(h + w + 1) * HC] * att).astype(BF16))
    gated = jnp.concatenate(gated, axis=0)
    update = dot(gated, wo_ref[...], TN)
    of[0, pl.ds(r, seqs, stride=8), :] = update[:, :128]
    of[1, pl.ds(r, seqs, stride=8), :] = update[:, 128:]

    @pl.when(r == pl.num_programs(0) - 1)
    def _():
        for k, o_ref in enumerate((oa, ob)):
            sl = slice(k * part * 8, (k + 1) * part * 8)
            o_ref[:, :128] = of[0, sl, :].astype(BF16)
            o_ref[:, 128:] = of[1, sl, :].astype(BF16)


def attention(which, blocks, weights, waits):
    count, part, width = blocks[0].shape
    full = pl.BlockSpec((256, 256), lambda r: (0, 0))
    seqs = 4 * part
    return pl.pallas_call(
        lambda *refs: attention_kernel(which, len(waits), *refs),
        grid=(count,),
        in_specs=[pl.BlockSpec((1, part, width), lambda r: (r, 0, 0))] * 4 + [full] * 5 + after(*waits),
        out_specs=[pl.BlockSpec((part * count, width), lambda r: (0, 0))] * 2,
        out_shape=[jax.ShapeDtypeStruct((part * count, width), BF16)] * 2,
        scratch_shapes=[pltpu.VMEM((2, 2 * part * count, 128), F32)],
        cost_estimate=pl.CostEstimate(
            flops=count * (seqs * seqs * 256 * 9 + 2 * seqs * 256 * 256 * 4),
            transcendentals=count * HEADS * seqs * seqs // 2,
            bytes_accessed=4 * count * seqs * width,
        ),
    )(*blocks, *weights, *waits)


def pair_kernel(scaling, i_ref, *refs):
    l_refs, (n_ref, f_ref, w_ref) = refs[:4], refs[4:7]
    o_ref, scr = refs[-2:]
    _, count, _, seqs = l_refs[0].shape
    rows = 8 * count
    left = jnp.concatenate([l[b].reshape(count * 32, seqs) for b in range(2) for l in l_refs], axis=0)
    for n in range(8):
        lanes = slice(n * 128, (n + 1) * 128)
        src = [
            jnp.concatenate([x[2 * b + h, :, lanes] for h in range(2) for x in (n_ref, f_ref)], axis=0)
            for b in range(4)
        ]
        right = jnp.concatenate([x[:, e * 32:(e + 1) * 32] for e in range(4) for x in src], axis=1)
        o = dot(left, right, NN).astype(BF16)
        for i in range(rows):
            for e in range(4):
                row = (n * 4 + e) * 32
                scr[i, row:row + 32, :] = o[i * 32:(i + 1) * 32, e * 128:(e + 1) * 128]
    at = i_ref[0]
    for k in range(rows // 2):
        rhs = jnp.concatenate([scr[2 * k], scr[2 * k + 1]], axis=1)
        t = dot(w_ref[...], rhs, NN) * scaling
        for u in range(2):
            i = 2 * k + u
            o_ref[at ^ (i // count), i % count] = t[:, u * 128:(u + 1) * 128].T.astype(BF16)


def pair_block(index, left, near, far, w_t, part, parts, scaling, waits):
    seqs = left[0].shape[-1]
    count = 8 // parts
    half = pl.BlockSpec(near.shape, lambda g: (0, 0, 0))
    return pl.pallas_call(
        lambda *refs: pair_kernel(scaling, *refs),
        grid=(1,),
        in_specs=[pl.BlockSpec(memory_space=pltpu.SMEM)]
        + [pl.BlockSpec((2, count, 32, seqs), lambda g: (0, part, 0, 0))] * 4
        + [half, half, pl.BlockSpec((128, 1024), lambda g: (0, 0))] + after(*waits),
        out_specs=pl.BlockSpec((8, count, 128, 128), lambda g: (0, 0, 0, 0)),
        out_shape=jax.ShapeDtypeStruct((8, count, 128, 128), BF16),
        scratch_shapes=[pltpu.VMEM((8 * count, 1024, 128), BF16)],
        cost_estimate=pl.CostEstimate(
            flops=(2 * 256 * 4096 * seqs + 2 * 8 * 128 * 128 * 1024) * count,
            transcendentals=0,
            bytes_accessed=2 * (4096 + 512) * seqs,
        ),
    )(index, *left, near, far, w_t, *waits)


def place_update(q, blocks):
    seqs, own, width = blocks[0].shape

    def kernel(q_ref, b0, b1, b2, b3, o_ref):
        q = q_ref[0]
        for k, b in enumerate((b0, b1, b2, b3)):
            o_ref[:, q ^ k] = b[...]

    vmem = pl.BlockSpec(memory_space=pltpu.VMEM)
    out = pl.pallas_call(
        kernel,
        in_specs=[pl.BlockSpec(memory_space=pltpu.SMEM)] + [vmem] * 4,
        out_specs=vmem,
        out_shape=jax.ShapeDtypeStruct((seqs, 4, own, width), BF16),
        cost_estimate=pl.CostEstimate(flops=300_000_000, transcendentals=0, bytes_accessed=16 * seqs * own * width),
        name="place_update",
    )(q, *blocks)
    return out.reshape(seqs, 4 * own, width)


def place_pair(col, got, prior, part, parts):
    count = 8 // parts

    def kernel(c_ref, g_ref, *refs):
        o_ref = refs[-1]
        for b in range(4):
            v = c_ref[0] ^ b
            a = (v % 2) * 2 + v // 2
            for k in range(8):
                o_ref[:, a, k] = g_ref[k, :, b]

    shape = (8, 4, 8, 32, 128)
    more = [] if prior is None else [prior]
    return pl.pallas_call(
        kernel,
        grid=(1,),
        in_specs=[
            pl.BlockSpec(memory_space=pltpu.SMEM),
            pl.BlockSpec((8, count, 4, 32, 128), lambda g: (0, 0, 0, 0, 0)),
        ] + after(*more),
        out_specs=pl.BlockSpec((count, *shape[1:]), lambda g: (part, 0, 0, 0, 0)),
        out_shape=jax.ShapeDtypeStruct(shape, BF16),
        input_output_aliases={2: 0} if more else {},
        cost_estimate=pl.CostEstimate(flops=300_000_000, transcendentals=0, bytes_accessed=4_000_000),
        name="place_pair",
    )(col, got.reshape(8, count, 4, 32, 128), *more)


def swap(x, axes, k):
    n = lax.axis_size(axes)
    return lax.ppermute(x, axes, [(j, j ^ k) for j in range(n)])


def layer(alignment, query_weight, w_keyval, w_gate, output_weight, w_factors, w_pair_out):
    seqs, residues, width = alignment.shape
    own = residues // 4
    total = seqs * 4
    q1 = lax.axis_index(SEQ).astype(jnp.int32)[None]
    row = lax.axis_index(ROWS).astype(jnp.int32)[None]
    col = lax.axis_index(("yh", "xl")).astype(jnp.int32)[None]
    weights = (query_weight.T, w_keyval[:, :256], w_keyval[:, 256:].T, w_gate.T, output_weight)
    w_t = w_pair_out.reshape(32, 32, 128).transpose(2, 1, 0).reshape(128, 1024)

    normed, lefts, right = front(q1, alignment.reshape(seqs * residues, width), w_factors.T)
    pieces = [lefts[0]] + [swap(lefts[k], SEQ, k) for k in (1, 2, 3)]
    x4 = jnp.stack([right, swap(right, XY, 1), swap(right, XY, 4), swap(right, XY, 5)])
    blocks = [normed[0]] + [swap(normed[k], SEQ, k) for k in (1, 2, 3)]
    near = jnp.concatenate([x4, swap(x4, XY, 2)], axis=0)
    left = merge_left(pieces)
    left2 = jnp.stack([left, swap(left, ROWS, 4)])
    left4 = [left2] + [swap(left2, ROWS, k) for k in (1, 2, 3)]
    far = swap(near, ("c",), 1)

    scaling = 1.0 / total
    u2, u3 = attention(2, blocks, weights, (left2, x4))
    backs = [None, None, swap(u2, SEQ, 2), swap(u3, SEQ, 3)]
    out0 = pair_block(row, left4, near, far, w_t, 0, 2, scaling, (u2,))
    got0 = lax.all_to_all(out0, ROWS, 0, 0)
    out1 = pair_block(row, left4, near, far, w_t, 1, 2, scaling, (out0,))
    got1 = lax.all_to_all(out1, ROWS, 0, 0)
    u0, u1 = attention(0, blocks, weights, (out1,))
    backs[0], backs[1] = u0, swap(u1, SEQ, 1)
    pair = place_pair(col, got0, None, 0, 2)
    pair = place_pair(col, got1, pair, 1, 2)
    alignment_update = place_update(q1, [b.reshape(seqs, own, width) for b in backs])
    return alignment_update, pair.reshape(8, 1024, 128)


def solution(mesh):
    split = Mesh(
        mesh.devices.reshape(2, 2, 2, 4, 2, 2), ("xl", "yh", "yl", "z", "xh", "c")
    )
    res = ("xl", "yh", "yl", "z")
    in_specs = (P(SEQ, res, None), P(), P(), P(), P(), P(), P())
    out_specs = (P(SEQ, res, None), P((*res, *SEQ), None, None))
    return jax.shard_map(layer, mesh=split, in_specs=in_specs, out_specs=out_specs, check_vma=False)
```

```python
import math

import jax
import jax.numpy as jnp
from jax import lax
from jax.experimental import pallas as pl
from jax.experimental.pallas import tpu as pltpu
from jax.sharding import Mesh
from jax.sharding import PartitionSpec as P


HEADS = 8
HC = 32
EPS = 1e-05
SEQ = ("xh", "c")
ROWS = ("yl", "z")
XY = ("xl", "yh", "xh")
SPLIT = 2
AT_ONCE = 2
NT = (((1,), (1,)), ((), ()))
NN = (((1,), (0,)), ((), ()))
TN = (((0,), (0,)), ((), ()))
TT = (((0,), (1,)), ((), ()))
F32 = jnp.float32
BF16 = jnp.bfloat16


def dot(a, b, dims):
    return lax.dot_general(a, b, dims, preferred_element_type=F32)


def after(*arrays):
    return [pl.BlockSpec(memory_space=pl.ANY)] * len(arrays)


def front_kernel(x_ref, wf_ref, n0, n1, n2, n3, l0, l1, l2, l3, r_ref, nf, nb, lf, rf, lb):
    rows = x_ref.shape[0]
    seqs = rows // 32
    step = 256

    def one(n, _):
        at = pl.ds(pl.multiple_of(n * step, step), step)
        v = x_ref[at, :].astype(F32)
        v = v - jnp.mean(v, axis=-1, keepdims=True)
        spread = jnp.mean(v * v, axis=-1, keepdims=True)
        y = v * lax.rsqrt(spread + EPS)
        nf[0, at, :] = y[:, :128]
        nf[1, at, :] = y[:, 128:]
        return 0

    lax.fori_loop(0, rows // step, one, 0)
    for r in range(32):
        at = pl.ds(r, seqs, stride=32)
        x = jnp.concatenate([nf[0, at, :], nf[1, at, :]], axis=1).astype(BF16)
        nb[r] = x
        f = dot(wf_ref[...], x, NT)
        lf[r * 32:(r + 1) * 32, :seqs] = f[:32]
        rf[pl.ds(r, 32, stride=32), :] = jnp.concatenate([f[32:], jnp.zeros((32, 128 - seqs), F32)], axis=1)
    for g in range(8):
        sl = slice(g * 128, (g + 1) * 128)
        piece = rf[sl, :].T[:seqs].astype(BF16)
        for k in range(8):
            r_ref[k, :, sl] = piece
        lb[g // 2, :, (g % 2) * 128:(g % 2 + 1) * 128] = lf[sl, :].T[:seqs].astype(BF16)
    q = lax.axis_index(SEQ)
    for k, (n_ref, l_ref) in enumerate(((n0, l0), (n1, l1), (n2, l2), (n3, l3))):
        for r in range(8):
            n_ref[r] = nb[(q ^ k) * 8 + r]
        l_ref[...] = lb[q ^ k]


def front(x, wf_t):
    rows = x.shape[0]
    seqs = rows // 32
    vmem = pl.BlockSpec(memory_space=pltpu.VMEM)
    outs = pl.pallas_call(
        front_kernel,
        in_specs=[vmem, vmem],
        out_shape=[jax.ShapeDtypeStruct((8, seqs, 256), BF16)] * 4
        + [jax.ShapeDtypeStruct((seqs, 256), BF16)] * 4
        + [jax.ShapeDtypeStruct((8, seqs, 1024), BF16)],
        scratch_shapes=[
            pltpu.VMEM((2, rows, 128), F32),
            pltpu.VMEM((32, seqs, 256), BF16),
            pltpu.VMEM((1024, 128), F32),
            pltpu.VMEM((1024, 128), F32),
            pltpu.VMEM((4, seqs, 256), BF16),
        ],
        cost_estimate=pl.CostEstimate(flops=800_000_000, transcendentals=rows, bytes_accessed=4 * rows * 256),
        name="front",
    )(x, wf_t)
    return outs[:4], outs[4:8], outs[8]


def merge_left(pieces):
    seqs = pieces[0].shape[0] * 4

    def kernel(p0, p1, p2, p3, o_ref):
        x = jnp.concatenate([p0[...], p1[...], p2[...], p3[...]], axis=0).astype(F32)
        o_ref[...] = x.T.astype(BF16)

    vmem = pl.BlockSpec(memory_space=pltpu.VMEM)
    out = pl.pallas_call(
        kernel,
        in_specs=[vmem] * 4,
        out_shape=jax.ShapeDtypeStruct((256, seqs), BF16),
        cost_estimate=pl.CostEstimate(flops=100_000_000, transcendentals=0, bytes_accessed=4 * 256 * seqs),
        name="merge_left",
    )(*pieces)
    return out.reshape(8, 32, seqs)


def attend(mine, keys, v_t, wq, wg, wo):
    seqs = mine.shape[0]
    q_t = dot(wq, mine, TT)
    q_t = jnp.concatenate([q_t, q_t], axis=1)
    first = lax.broadcasted_iota(jnp.int32, q_t.shape, 1) < seqs
    q_even = jnp.where(first, q_t, 0.0).astype(BF16)
    q_odd = jnp.where(first, 0.0, q_t).astype(BF16)
    g_t = jax.nn.sigmoid(dot(wg, mine, TT))
    ones = jnp.ones((16, keys.shape[0]), BF16)
    scale = math.log2(math.e) / math.sqrt(HC)
    gated = []

    def spread(h):
        parts = [q_even[h * HC:(h + 1) * HC], q_odd[(h + 1) * HC:(h + 2) * HC]]
        if h:
            parts.insert(0, jnp.zeros((h * HC, 2 * seqs), BF16))
        if h < HEADS - 2:
            parts.append(jnp.zeros(((HEADS - 2 - h) * HC, 2 * seqs), BF16))
        return jnp.concatenate(parts, axis=0)

    for p in range(HEADS // 4):
        rhs = jnp.concatenate([spread(4 * p), spread(4 * p + 2)], axis=1)
        scores = dot(keys, rhs, NN)
        weights = jnp.exp2(scores * scale).astype(BF16)
        tiles = []
        for u in range(3):
            h = 4 * p + u
            lhs = jnp.concatenate([v_t[h * HC:(h + 2) * HC], ones], axis=0)
            out = dot(lhs, weights[:, u * 256:(u + 1) * 256], NN)
            tiles.append(out[:2 * HC] / out[2 * HC:2 * HC + 1])
        lo, hi = slice(0, HC), slice(HC, 2 * HC)
        heads = (
            tiles[0][lo, :192],
            jnp.concatenate([tiles[0][hi, 192:], tiles[1][lo, :128]], axis=1),
            jnp.concatenate([tiles[1][hi, 128:], tiles[2][lo, :64]], axis=1),
            tiles[2][hi, 64:],
        )
        for u, att in enumerate(heads):
            h = 4 * p + u
            gated.append((g_t[h * HC:(h + 1) * HC] * att).astype(BF16))
    gated = jnp.concatenate(gated, axis=0)
    return dot(gated, wo, TN)


def finish(g, of, part, o_refs):
    @pl.when(g == pl.num_programs(0) - 1)
    def _():
        for k, o_ref in enumerate(o_refs):
            sl = slice(k * part * 8, (k + 1) * part * 8)
            o_ref[:, :128] = of[0, sl, :].astype(BF16)
            o_ref[:, 128:] = of[1, sl, :].astype(BF16)


def far_kernel(n_wait, *refs):
    x_refs, (wq_ref, wkv_ref, wg_ref, wo_ref) = refs[:4], refs[4:8]
    oa, ob, k_ref, v_ref, of = refs[8 + n_wait:]
    g = pl.program_id(0)
    at_once, part = x_refs[0].shape[:2]
    for n in range(at_once):
        x = jnp.concatenate([b[n] for b in x_refs], axis=0)
        keys = dot(x, wkv_ref[:, :256], NN).astype(BF16)
        v_t = dot(wkv_ref[:, 256:], x, TT).astype(BF16)
        k_ref[n] = keys
        v_ref[n] = v_t
        update = attend(x[2 * part:], keys, v_t, wq_ref[...], wg_ref[...], wo_ref[...])
        rows = pl.ds(g * at_once + n, 2 * part, stride=8)
        of[0, rows, :] = update[:, :128]
        of[1, rows, :] = update[:, 128:]
    finish(g, of, part, (oa, ob))


def near_kernel(n_wait, *refs):
    x_refs, (k_ref, v_ref), (wq_ref, wg_ref, wo_ref) = refs[:2], refs[2:4], refs[4:7]
    oa, ob, of = refs[7 + n_wait:]
    g = pl.program_id(0)
    at_once, part = x_refs[0].shape[:2]
    for n in range(at_once):
        mine = jnp.concatenate([b[n] for b in x_refs], axis=0)
        update = attend(mine, k_ref[n], v_ref[n], wq_ref[...], wg_ref[...], wo_ref[...])
        rows = pl.ds(g * at_once + n, 2 * part, stride=8)
        of[0, rows, :] = update[:, :128]
        of[1, rows, :] = update[:, 128:]
    finish(g, of, part, (oa, ob))


def attention(blocks, kept, weights, waits):
    count, part, width = blocks[0].shape
    seqs = 4 * part
    full = pl.BlockSpec((256, 256), lambda r: (0, 0))
    by_residue = lambda *tail: pl.BlockSpec((AT_ONCE, *tail), lambda r: (r, 0, 0))
    out_specs = [pl.BlockSpec((part * count, width), lambda r: (0, 0))] * 2
    out_shape = [jax.ShapeDtypeStruct((part * count, width), BF16)] * 2
    wq, wkv, wg, wo = weights
    if kept is None:
        kernel = far_kernel
        operands = (*blocks, wq, wkv, wg, wo)
        in_specs = [by_residue(part, width)] * 4 + [full, pl.BlockSpec((256, 512), lambda r: (0, 0)), full, full]
        out_specs += [by_residue(seqs, width), by_residue(width, seqs)]
        out_shape += [
            jax.ShapeDtypeStruct((count, seqs, width), BF16),
            jax.ShapeDtypeStruct((count, width, seqs), BF16),
        ]
    else:
        kernel = near_kernel
        operands = (*blocks[:2], *kept, wq, wg, wo)
        in_specs = [by_residue(part, width)] * 2 + [by_residue(seqs, width), by_residue(width, seqs)] + [full] * 3
    return pl.pallas_call(
        lambda *refs: kernel(len(waits), *refs),
        grid=(count // AT_ONCE,),
        in_specs=in_specs + after(*waits),
        out_specs=out_specs,
        out_shape=out_shape,
        scratch_shapes=[pltpu.VMEM((2, 2 * part * count, 128), F32)],
        cost_estimate=pl.CostEstimate(
            flops=count * (seqs * seqs * 256 * 9 + 2 * seqs * 256 * 256 * 4),
            transcendentals=count * HEADS * seqs * seqs // 2,
            bytes_accessed=4 * count * seqs * width,
        ),
    )(*operands, *waits)


def pair_kernel(scaling, r0, count, *refs):
    l_refs, right_refs, w_ref = refs[:8], refs[8:10], refs[10]
    o_ref, scr = refs[-2:]
    seqs = l_refs[0].shape[-1]
    rows = 8 * count
    xy = lax.axis_index(XY)
    left = jnp.concatenate([l[r0:r0 + count].reshape(count * 32, seqs) for l in l_refs], axis=0)
    for n in range(8):
        lanes = slice(n * 128, (n + 1) * 128)
        src = []
        for b in range(4):
            m = (b % 2) * 4 + (b // 2) * 2
            src.append(
                jnp.concatenate([x[xy ^ (m + h), :, lanes] for h in range(2) for x in right_refs], axis=0)
            )
        right = jnp.concatenate([x[:, e * 32:(e + 1) * 32] for e in range(4) for x in src], axis=1)
        o = dot(left, right, NN).astype(BF16)
        for i in range(rows):
            for e in range(4):
                row = (n * 4 + e) * 32
                scr[i, row:row + 32, :] = o[i * 32:(i + 1) * 32, e * 128:(e + 1) * 128]
    at = lax.axis_index(ROWS)
    for k in range(rows // 2):
        rhs = jnp.concatenate([scr[2 * k], scr[2 * k + 1]], axis=1)
        t = dot(w_ref[...], rhs, NN) * scaling
        for u in range(2):
            i = 2 * k + u
            o_ref[at ^ (i // count), i % count] = t[:, u * 128:(u + 1) * 128].T.astype(BF16)


def pair_block(left, rights, w_t, r0, count, scaling, waits):
    seqs = left[0].shape[-1]
    vmem = pl.BlockSpec(memory_space=pltpu.VMEM)
    return pl.pallas_call(
        lambda *refs: pair_kernel(scaling, r0, count, *refs),
        in_specs=[vmem] * 11 + after(*waits),
        out_specs=vmem,
        out_shape=jax.ShapeDtypeStruct((8, count, 128, 128), BF16),
        scratch_shapes=[pltpu.VMEM((8 * count, 1024, 128), BF16)],
        cost_estimate=pl.CostEstimate(
            flops=(2 * 256 * 4096 * seqs + 2 * 8 * 128 * 128 * 1024) * count,
            transcendentals=0,
            bytes_accessed=2 * (4096 + 512) * seqs,
        ),
    )(*left, *rights, w_t, *waits)


def place(blocks, wheres, shape, prior):
    n = len(blocks)
    more = [] if prior is None else [prior]

    def kernel(*refs):
        ins, out, sems = refs[:n], refs[-2], refs[-1]
        pairs = [p for b, where in zip(ins, wheres) for p in where(b, out)]
        copies = [pltpu.make_async_copy(a, to, sems.at[k]) for k, (a, to) in enumerate(pairs)]
        for c in copies:
            c.start()
        for c in copies:
            c.wait()

    hbm = pl.BlockSpec(memory_space=pltpu.HBM)
    return pl.pallas_call(
        kernel,
        in_specs=[pl.BlockSpec(memory_space=pltpu.VMEM)] * n + [hbm] * len(more),
        out_specs=hbm,
        out_shape=jax.ShapeDtypeStruct(shape, BF16),
        scratch_shapes=[pltpu.SemaphoreType.DMA((32,))],
        input_output_aliases={n: 0} if more else {},
        cost_estimate=pl.CostEstimate(flops=300_000_000, transcendentals=0, bytes_accessed=4_000_000),
    )(*blocks, *more)


def place_update(blocks):
    seqs, own, width = blocks[0].shape

    def to_group(k):
        return lambda b, out: [(b, out.at[:, lax.axis_index(SEQ) ^ k])]

    out = place(blocks, [to_group(k) for k in range(4)], (seqs, 4, own, width), None)
    return out.reshape(seqs, 4 * own, width)


def place_pair(got, prior, r0):
    count = got.shape[1]

    def where(g, out):
        pairs = []
        for b in range(4):
            v = lax.axis_index(("yh", "xl")) ^ b
            a = (v % 2) * 2 + v // 2
            for k in range(8):
                pairs.append((g.at[k, :, b], out.at[pl.ds(r0, count), a, k]))
        return pairs

    return place([got.reshape(8, count, 4, 32, 128)], [where], (8, 4, 8, 32, 128), prior)


def swap(x, axes, k):
    n = lax.axis_size(axes)
    return lax.ppermute(x, axes, [(j, j ^ k) for j in range(n)])


def layer(alignment, query_weight, w_keyval, w_gate, output_weight, w_factors, w_pair_out):
    seqs, residues, width = alignment.shape
    own = residues // 4
    total = seqs * 4
    normed, lefts, right = front(alignment.reshape(seqs * residues, width), w_factors.T)
    blocks = [normed[0]] + [swap(normed[k], SEQ, k) for k in (1, 2, 3)]
    near = lax.all_to_all(right, XY, 0, 0)
    pieces = [lefts[0]] + [swap(lefts[k], SEQ, k) for k in (1, 2, 3)]
    left = merge_left(pieces)
    left_y = swap(left, ROWS, 4)
    left8 = [left] + [swap(left, ROWS, k) for k in (1, 2, 3)]
    left8 += [left_y] + [swap(left_y, ROWS, k) for k in (1, 2, 3)]
    rights = [near, swap(near, ("c",), 1)]

    w_pair_out, left = lax.optimization_barrier((w_pair_out, left))
    weights = (query_weight, w_keyval, w_gate, output_weight)
    w_t = w_pair_out.reshape(32, 32, 128).transpose(2, 1, 0).reshape(128, 1024)
    scaling = 1.0 / total
    u2, u3, *kept = attention(blocks, None, weights, (left_y,))
    backs = [None, None, swap(u2, SEQ, 2), swap(u3, SEQ, 3)]
    out0 = pair_block(left8, rights, w_t, 0, SPLIT, scaling, (u2,))
    got0 = lax.all_to_all(out0, ROWS, 0, 0)
    out1 = pair_block(left8, rights, w_t, SPLIT, 8 - SPLIT, scaling, (out0,))
    got1 = lax.all_to_all(out1, ROWS, 0, 0)
    pair = place_pair(got0, None, 0)
    u0, u1 = attention(blocks, kept, weights, (out1, pair))
    backs[0], backs[1] = u0, swap(u1, SEQ, 1)
    alignment_update = place_update([b.reshape(seqs, own, width) for b in backs])
    pair = place_pair(got1, pair, SPLIT)
    return alignment_update, pair.reshape(8, 1024, 128)


def solution(mesh):
    split = Mesh(
        mesh.devices.reshape(2, 2, 2, 4, 2, 2), ("xl", "yh", "yl", "z", "xh", "c")
    )
    res = ("xl", "yh", "yl", "z")
    in_specs = (P(SEQ, res, None), P(), P(), P(), P(), P(), P())
    out_specs = (P(SEQ, res, None), P((*res, *SEQ), None, None))
    return jax.shard_map(layer, mesh=split, in_specs=in_specs, out_specs=out_specs, check_vma=False)
```

```python
import math

import jax
import jax.numpy as jnp
from jax import lax
from jax.experimental import pallas as pl
from jax.experimental.pallas import tpu as pltpu
from jax.sharding import Mesh
from jax.sharding import PartitionSpec as P


HEADS = 8
HC = 32
EPS = 1e-05
SEQ = ("xh", "c")
ROWS = ("yl", "z")
XY = ("xl", "yh", "xh")
SPLIT = 2
PAD = 40
AT_ONCE = 4
NT = (((1,), (1,)), ((), ()))
NN = (((1,), (0,)), ((), ()))
TN = (((0,), (0,)), ((), ()))
TT = (((0,), (1,)), ((), ()))
F32 = jnp.float32
BF16 = jnp.bfloat16


def dot(a, b, dims):
    return lax.dot_general(a, b, dims, preferred_element_type=F32)


def after(*arrays):
    return [pl.BlockSpec(memory_space=pl.ANY)] * len(arrays)


def front_kernel(x_ref, wf_ref, n0, n1, n2, n3, l0, l1, l2, l3, r_ref, nf, nb, lf, rf, lb):
    rows = x_ref.shape[0]
    seqs = rows // 32
    step = 256

    def one(n, _):
        at = pl.ds(pl.multiple_of(n * step, step), step)
        v = x_ref[at, :].astype(F32)
        v = v - jnp.mean(v, axis=-1, keepdims=True)
        spread = jnp.mean(v * v, axis=-1, keepdims=True)
        y = v * lax.rsqrt(spread + EPS)
        for j in range(step // 32):
            to = pl.ds(pl.multiple_of((n * (step // 32) + j) * PAD, 8), 32)
            nf[0, to, :] = y[j * 32:(j + 1) * 32, :128]
            nf[1, to, :] = y[j * 32:(j + 1) * 32, 128:]
        return 0

    lax.fori_loop(0, rows // step, one, 0)
    for r in range(32):
        at = pl.ds(r, seqs, stride=PAD)
        x = jnp.concatenate([nf[0, at, :], nf[1, at, :]], axis=1).astype(BF16)
        nb[r] = x
        f = dot(wf_ref[...], x, NT)
        lf[r * 32:(r + 1) * 32, :seqs] = f[:32]
        rf[pl.ds(r, 32, stride=PAD), :] = jnp.concatenate([f[32:], jnp.zeros((32, 128 - seqs), F32)], axis=1)
    for g in range(8):
        sl = slice(g * 128, (g + 1) * 128)
        piece = jnp.concatenate([rf[e * PAD:e * PAD + 32, :] for e in range(4 * g, 4 * g + 4)], axis=0)
        piece = piece.T[:seqs].astype(BF16)
        for k in range(8):
            r_ref[k, :, sl] = piece
        lb[g // 2, :, (g % 2) * 128:(g % 2 + 1) * 128] = lf[sl, :].T[:seqs].astype(BF16)
    q = lax.axis_index(SEQ)
    for k, (n_ref, l_ref) in enumerate(((n0, l0), (n1, l1), (n2, l2), (n3, l3))):
        for r in range(8):
            n_ref[r] = nb[(q ^ k) * 8 + r]
        l_ref[...] = lb[q ^ k]


def front(x, wf_t):
    rows = x.shape[0]
    seqs = rows // 32
    vmem = pl.BlockSpec(memory_space=pltpu.VMEM)
    outs = pl.pallas_call(
        front_kernel,
        in_specs=[vmem, vmem],
        out_shape=[jax.ShapeDtypeStruct((8, seqs, 256), BF16)] * 4
        + [jax.ShapeDtypeStruct((seqs, 256), BF16)] * 4
        + [jax.ShapeDtypeStruct((8, seqs, 1024), BF16)],
        scratch_shapes=[
            pltpu.VMEM((2, seqs * PAD, 128), F32),
            pltpu.VMEM((32, seqs, 256), BF16),
            pltpu.VMEM((1024, 128), F32),
            pltpu.VMEM((32 * PAD, 128), F32),
            pltpu.VMEM((4, seqs, 256), BF16),
        ],
        cost_estimate=pl.CostEstimate(flops=800_000_000, transcendentals=rows, bytes_accessed=4 * rows * 256),
        name="front",
    )(x, wf_t)
    return outs[:4], outs[4:8], outs[8]


def merge_left(pieces):
    seqs = pieces[0].shape[0] * 4

    def kernel(p0, p1, p2, p3, o_ref):
        x = jnp.concatenate([p0[...], p1[...], p2[...], p3[...]], axis=0).astype(F32)
        o_ref[...] = x.T.astype(BF16)

    vmem = pl.BlockSpec(memory_space=pltpu.VMEM)
    out = pl.pallas_call(
        kernel,
        in_specs=[vmem] * 4,
        out_shape=jax.ShapeDtypeStruct((256, seqs), BF16),
        cost_estimate=pl.CostEstimate(flops=100_000_000, transcendentals=0, bytes_accessed=4 * 256 * seqs),
        name="merge_left",
    )(*pieces)
    return out.reshape(8, 32, seqs)


def attend(items, wq, wg, wo):
    seqs = items[0][0].shape[0]
    ones = jnp.ones((16, items[0][1].shape[0]), BF16)
    scale = math.log2(math.e) / math.sqrt(HC)
    quads = HEADS // 4
    ready = []
    for mine, keys, v_t in items:
        q_t = dot(wq, mine, TT)
        q_t = jnp.concatenate([q_t, q_t], axis=1)
        first = lax.broadcasted_iota(jnp.int32, q_t.shape, 1) < seqs
        q_even = jnp.where(first, q_t, 0.0).astype(BF16)
        q_odd = jnp.where(first, 0.0, q_t).astype(BF16)
        ready.append((q_even, q_odd, jax.nn.sigmoid(dot(wg, mine, TT))))

    def spread(n, h):
        q_even, q_odd, _ = ready[n]
        parts = [q_even[h * HC:(h + 1) * HC], q_odd[(h + 1) * HC:(h + 2) * HC]]
        if h:
            parts.insert(0, jnp.zeros((h * HC, 2 * seqs), BF16))
        if h < HEADS - 2:
            parts.append(jnp.zeros(((HEADS - 2 - h) * HC, 2 * seqs), BF16))
        return jnp.concatenate(parts, axis=0)

    def scores_of(n, p):
        rhs = jnp.concatenate([spread(n, 4 * p), spread(n, 4 * p + 2)], axis=1)
        return dot(items[n][1], rhs, NN)

    order = [(n, p) for n in range(len(items)) for p in range(quads)]
    gated = [[] for _ in items]
    updates = []
    ahead = scores_of(*order[0])
    for at, (n, p) in enumerate(order):
        scores = ahead
        if at + 1 < len(order):
            ahead = scores_of(*order[at + 1])
        weights = jnp.exp2(scores * scale).astype(BF16)
        v_t, g_t = items[n][2], ready[n][2]
        tiles = []
        for u in range(3):
            h = 4 * p + u
            lhs = jnp.concatenate([v_t[h * HC:(h + 2) * HC], ones], axis=0)
            out = dot(lhs, weights[:, u * 256:(u + 1) * 256], NN)
            tiles.append(out[:2 * HC] / out[2 * HC:2 * HC + 1])
        lo, hi = slice(0, HC), slice(HC, 2 * HC)
        heads = (
            tiles[0][lo, :192],
            jnp.concatenate([tiles[0][hi, 192:], tiles[1][lo, :128]], axis=1),
            jnp.concatenate([tiles[1][hi, 128:], tiles[2][lo, :64]], axis=1),
            tiles[2][hi, 64:],
        )
        for u, att in enumerate(heads):
            h = 4 * p + u
            gated[n].append((g_t[h * HC:(h + 1) * HC] * att).astype(BF16))
        if p == quads - 1:
            updates.append(dot(jnp.concatenate(gated[n], axis=0), wo, TN))
    return updates


def finish(g, of, part, o_refs):
    @pl.when(g == pl.num_programs(0) - 1)
    def _():
        for k, o_ref in enumerate(o_refs):
            sl = slice(k * part * 8, (k + 1) * part * 8)
            o_ref[:, :128] = of[0, sl, :].astype(BF16)
            o_ref[:, 128:] = of[1, sl, :].astype(BF16)


def far_kernel(n_wait, *refs):
    x_refs, (wq_ref, wkv_ref, wg_ref, wo_ref) = refs[:4], refs[4:8]
    oa, ob, k_ref, v_ref, of = refs[8 + n_wait:]
    g = pl.program_id(0)
    at_once, part = x_refs[0].shape[:2]
    items = []
    for n in range(at_once):
        x = jnp.concatenate([b[n] for b in x_refs], axis=0)
        keys = dot(x, wkv_ref[:, :256], NN).astype(BF16)
        v_t = dot(wkv_ref[:, 256:], x, TT).astype(BF16)
        k_ref[n] = keys
        v_ref[n] = v_t
        items.append((x[2 * part:], keys, v_t))
    for n, update in enumerate(attend(items, wq_ref[...], wg_ref[...], wo_ref[...])):
        rows = pl.ds(g * at_once + n, 2 * part, stride=8)
        of[0, rows, :] = update[:, :128]
        of[1, rows, :] = update[:, 128:]
    finish(g, of, part, (oa, ob))


def near_kernel(n_wait, *refs):
    x_refs, (k_ref, v_ref), (wq_ref, wg_ref, wo_ref) = refs[:2], refs[2:4], refs[4:7]
    oa, ob, of = refs[7 + n_wait:]
    g = pl.program_id(0)
    at_once, part = x_refs[0].shape[:2]
    items = [
        (jnp.concatenate([b[n] for b in x_refs], axis=0), k_ref[n], v_ref[n]) for n in range(at_once)
    ]
    for n, update in enumerate(attend(items, wq_ref[...], wg_ref[...], wo_ref[...])):
        rows = pl.ds(g * at_once + n, 2 * part, stride=8)
        of[0, rows, :] = update[:, :128]
        of[1, rows, :] = update[:, 128:]
    finish(g, of, part, (oa, ob))


def attention(blocks, kept, weights, waits):
    count, part, width = blocks[0].shape
    seqs = 4 * part
    full = pl.BlockSpec((256, 256), lambda r: (0, 0))
    by_residue = lambda *tail: pl.BlockSpec((AT_ONCE, *tail), lambda r: (r, 0, 0))
    out_specs = [pl.BlockSpec((part * count, width), lambda r: (0, 0))] * 2
    out_shape = [jax.ShapeDtypeStruct((part * count, width), BF16)] * 2
    wq, wkv, wg, wo = weights
    if kept is None:
        kernel = far_kernel
        operands = (*blocks, wq, wkv, wg, wo)
        in_specs = [by_residue(part, width)] * 4 + [full, pl.BlockSpec((256, 512), lambda r: (0, 0)), full, full]
        out_specs += [by_residue(seqs, width), by_residue(width, seqs)]
        out_shape += [
            jax.ShapeDtypeStruct((count, seqs, width), BF16),
            jax.ShapeDtypeStruct((count, width, seqs), BF16),
        ]
    else:
        kernel = near_kernel
        operands = (*blocks[:2], *kept, wq, wg, wo)
        in_specs = [by_residue(part, width)] * 2 + [by_residue(seqs, width), by_residue(width, seqs)] + [full] * 3
    return pl.pallas_call(
        lambda *refs: kernel(len(waits), *refs),
        grid=(count // AT_ONCE,),
        in_specs=in_specs + after(*waits),
        out_specs=out_specs,
        out_shape=out_shape,
        scratch_shapes=[pltpu.VMEM((2, 2 * part * count, 128), F32)],
        cost_estimate=pl.CostEstimate(
            flops=count * (seqs * seqs * 256 * 9 + 2 * seqs * 256 * 256 * 4),
            transcendentals=count * HEADS * seqs * seqs // 2,
            bytes_accessed=4 * count * seqs * width,
        ),
    )(*operands, *waits)


def pair_kernel(scaling, r0, count, *refs):
    l_refs, right_refs, w_ref = refs[:8], refs[8:10], refs[10]
    o_ref, scr = refs[-2:]
    seqs = l_refs[0].shape[-1]
    rows = 8 * count
    xy = lax.axis_index(XY)
    left = jnp.concatenate([l[r0:r0 + count].reshape(count * 32, seqs) for l in l_refs], axis=0)
    for n in range(8):
        lanes = slice(n * 128, (n + 1) * 128)
        src = []
        for b in range(4):
            m = (b % 2) * 4 + (b // 2) * 2
            src.append(
                jnp.concatenate([x[xy ^ (m + h), :, lanes] for h in range(2) for x in right_refs], axis=0)
            )
        right = jnp.concatenate([x[:, e * 32:(e + 1) * 32] for e in range(4) for x in src], axis=1)
        o = dot(left, right, NN).astype(BF16)
        for i in range(rows):
            for e in range(4):
                row = (n * 4 + e) * 32
                scr[i, row:row + 32, :] = o[i * 32:(i + 1) * 32, e * 128:(e + 1) * 128]
    at = lax.axis_index(ROWS)
    for k in range(rows // 2):
        rhs = jnp.concatenate([scr[2 * k], scr[2 * k + 1]], axis=1)
        t = dot(w_ref[...], rhs, NN) * scaling
        for u in range(2):
            i = 2 * k + u
            o_ref[at ^ (i // count), i % count] = t[:, u * 128:(u + 1) * 128].T.astype(BF16)


def pair_block(left, rights, w_t, r0, count, scaling, waits):
    seqs = left[0].shape[-1]
    vmem = pl.BlockSpec(memory_space=pltpu.VMEM)
    return pl.pallas_call(
        lambda *refs: pair_kernel(scaling, r0, count, *refs),
        in_specs=[vmem] * 11 + after(*waits),
        out_specs=vmem,
        out_shape=jax.ShapeDtypeStruct((8, count, 128, 128), BF16),
        scratch_shapes=[pltpu.VMEM((8 * count, 1024, 128), BF16)],
        cost_estimate=pl.CostEstimate(
            flops=(2 * 256 * 4096 * seqs + 2 * 8 * 128 * 128 * 1024) * count,
            transcendentals=0,
            bytes_accessed=2 * (4096 + 512) * seqs,
        ),
    )(*left, *rights, w_t, *waits)


def place(blocks, wheres, shape, prior):
    n = len(blocks)
    more = [] if prior is None else [prior]

    def kernel(*refs):
        ins, out, sems = refs[:n], refs[-2], refs[-1]
        pairs = [p for b, where in zip(ins, wheres) for p in where(b, out)]
        copies = [pltpu.make_async_copy(a, to, sems.at[k]) for k, (a, to) in enumerate(pairs)]
        for c in copies:
            c.start()
        for c in copies:
            c.wait()

    hbm = pl.BlockSpec(memory_space=pltpu.HBM)
    return pl.pallas_call(
        kernel,
        in_specs=[pl.BlockSpec(memory_space=pltpu.VMEM)] * n + [hbm] * len(more),
        out_specs=hbm,
        out_shape=jax.ShapeDtypeStruct(shape, BF16),
        scratch_shapes=[pltpu.SemaphoreType.DMA((32,))],
        input_output_aliases={n: 0} if more else {},
        cost_estimate=pl.CostEstimate(flops=300_000_000, transcendentals=0, bytes_accessed=4_000_000),
    )(*blocks, *more)


def place_update(blocks):
    seqs, own, width = blocks[0].shape

    def to_group(k):
        return lambda b, out: [(b, out.at[:, lax.axis_index(SEQ) ^ k])]

    out = place(blocks, [to_group(k) for k in range(4)], (seqs, 4, own, width), None)
    return out.reshape(seqs, 4 * own, width)


def place_pair(got, prior, r0):
    count = got.shape[1]
    shape = (8, 4, 8, 32, 128)
    more = [] if prior is None else [prior]

    def kernel(g_hbm, *refs):
        out, buf, in_sems, out_sems = refs[-4:]
        loads = [pltpu.make_async_copy(g_hbm.at[k], buf.at[k], in_sems.at[k]) for k in range(8)]
        for c in loads:
            c.start()
        stores = []
        for k in range(8):
            loads[k].wait()
            for b in range(4):
                v = lax.axis_index(("yh", "xl")) ^ b
                a = (v % 2) * 2 + v // 2
                to = out.at[pl.ds(r0, count), a, k]
                stores.append(pltpu.make_async_copy(buf.at[k, :, b], to, out_sems.at[4 * k + b]))
                stores[-1].start()
        for c in stores:
            c.wait()

    hbm = pl.BlockSpec(memory_space=pltpu.HBM)
    return pl.pallas_call(
        kernel,
        in_specs=[hbm] * (1 + len(more)),
        out_specs=hbm,
        out_shape=jax.ShapeDtypeStruct(shape, BF16),
        scratch_shapes=[
            pltpu.VMEM((8, count, 4, 32, 128), BF16),
            pltpu.SemaphoreType.DMA((8,)),
            pltpu.SemaphoreType.DMA((32,)),
        ],
        input_output_aliases={1: 0} if more else {},
        cost_estimate=pl.CostEstimate(flops=300_000_000, transcendentals=0, bytes_accessed=4_000_000),
    )(got.reshape(8, count, 4, 32, 128), *more)


def swap(x, axes, k):
    n = lax.axis_size(axes)
    return lax.ppermute(x, axes, [(j, j ^ k) for j in range(n)])


def layer(alignment, query_weight, w_keyval, w_gate, output_weight, w_factors, w_pair_out):
    seqs, residues, width = alignment.shape
    own = residues // 4
    total = seqs * 4
    normed, lefts, right = front(alignment.reshape(seqs * residues, width), w_factors.T)
    blocks = [normed[0]] + [swap(normed[k], SEQ, k) for k in (1, 2, 3)]
    near = lax.all_to_all(right, XY, 0, 0)
    pieces = [lefts[0]] + [swap(lefts[k], SEQ, k) for k in (1, 2, 3)]
    left = merge_left(pieces)
    left_y = swap(left, ROWS, 4)
    left8 = [left] + [swap(left, ROWS, k) for k in (1, 2, 3)]
    left8 += [left_y] + [swap(left_y, ROWS, k) for k in (1, 2, 3)]
    rights = [near, swap(near, ("c",), 1)]

    w_pair_out, left = lax.optimization_barrier((w_pair_out, left))
    weights = (query_weight, w_keyval, w_gate, output_weight)
    w_t = w_pair_out.reshape(32, 32, 128).transpose(2, 1, 0).reshape(128, 1024)
    scaling = 1.0 / total
    u2, u3, *kept = attention(blocks, None, weights, (left_y,))
    backs = [None, None, swap(u2, SEQ, 2), swap(u3, SEQ, 3)]
    out0 = pair_block(left8, rights, w_t, 0, SPLIT, scaling, (u2,))
    got0 = lax.all_to_all(out0, ROWS, 0, 0)
    out1 = pair_block(left8, rights, w_t, SPLIT, 8 - SPLIT, scaling, (out0,))
    got1 = lax.all_to_all(out1, ROWS, 0, 0)
    pair = place_pair(got0, None, 0)
    u0, u1 = attention(blocks, kept, weights, (out1, pair))
    backs[0], backs[1] = u0, swap(u1, SEQ, 1)
    alignment_update = place_update([b.reshape(seqs, own, width) for b in backs])
    pair = place_pair(got1, pair, SPLIT)
    return alignment_update, pair.reshape(8, 1024, 128)


def solution(mesh):
    split = Mesh(
        mesh.devices.reshape(2, 2, 2, 4, 2, 2), ("xl", "yh", "yl", "z", "xh", "c")
    )
    res = ("xl", "yh", "yl", "z")
    in_specs = (P(SEQ, res, None), P(), P(), P(), P(), P(), P())
    out_specs = (P(SEQ, res, None), P((*res, *SEQ), None, None))
    return jax.shard_map(layer, mesh=split, in_specs=in_specs, out_specs=out_specs, check_vma=False)
```

```python
import math

import jax
import jax.numpy as jnp
from jax import lax
from jax.experimental import pallas as pl
from jax.experimental.pallas import tpu as pltpu
from jax.sharding import Mesh
from jax.sharding import PartitionSpec as P


HEADS = 8
HC = 32
EPS = 1e-05
SEQ = ("xh", "c")
ROWS = ("yl", "z")
XY = ("xl", "yh", "xh")
SPLIT = 3
PAD = 40
AT_ONCE = 4
NT = (((1,), (1,)), ((), ()))
NN = (((1,), (0,)), ((), ()))
TN = (((0,), (0,)), ((), ()))
TT = (((0,), (1,)), ((), ()))
F32 = jnp.float32
BF16 = jnp.bfloat16


def dot(a, b, dims):
    return lax.dot_general(a, b, dims, preferred_element_type=F32)


def after(*arrays):
    return [pl.BlockSpec(memory_space=pl.ANY)] * len(arrays)


def front_kernel(x_ref, wf_ref, n0, n1, n2, n3, l0, l1, l2, l3, r_ref, nf, nb, lf, rf, lb):
    rows = x_ref.shape[0]
    seqs = rows // 32
    step = 256

    def one(n, _):
        at = pl.ds(pl.multiple_of(n * step, step), step)
        v = x_ref[at, :].astype(F32)
        v = v - jnp.mean(v, axis=-1, keepdims=True)
        spread = jnp.mean(v * v, axis=-1, keepdims=True)
        y = v * lax.rsqrt(spread + EPS)
        for j in range(step // 32):
            to = pl.ds(pl.multiple_of((n * (step // 32) + j) * PAD, 8), 32)
            nf[0, to, :] = y[j * 32:(j + 1) * 32, :128]
            nf[1, to, :] = y[j * 32:(j + 1) * 32, 128:]
        return 0

    lax.fori_loop(0, rows // step, one, 0)
    for r in range(32):
        at = pl.ds(r, seqs, stride=PAD)
        x = jnp.concatenate([nf[0, at, :], nf[1, at, :]], axis=1).astype(BF16)
        nb[r] = x
        f = dot(wf_ref[...], x, NT)
        lf[r * 32:(r + 1) * 32, :seqs] = f[:32]
        rf[pl.ds(r, 32, stride=PAD), :] = jnp.concatenate([f[32:], jnp.zeros((32, 128 - seqs), F32)], axis=1)
    for g in range(8):
        sl = slice(g * 128, (g + 1) * 128)
        piece = jnp.concatenate([rf[e * PAD:e * PAD + 32, :] for e in range(4 * g, 4 * g + 4)], axis=0)
        piece = piece.T[:seqs].astype(BF16)
        for k in range(8):
            r_ref[k, :, sl] = piece
        lb[g // 2, :, (g % 2) * 128:(g % 2 + 1) * 128] = lf[sl, :].T[:seqs].astype(BF16)
    q = lax.axis_index(SEQ)
    for k, (n_ref, l_ref) in enumerate(((n0, l0), (n1, l1), (n2, l2), (n3, l3))):
        for r in range(8):
            n_ref[r] = nb[(q ^ k) * 8 + r]
        l_ref[...] = lb[q ^ k]


def front(x, wf_t):
    rows = x.shape[0]
    seqs = rows // 32
    vmem = pl.BlockSpec(memory_space=pltpu.VMEM)
    outs = pl.pallas_call(
        front_kernel,
        in_specs=[vmem, vmem],
        out_shape=[jax.ShapeDtypeStruct((8, seqs, 256), BF16)] * 4
        + [jax.ShapeDtypeStruct((seqs, 256), BF16)] * 4
        + [jax.ShapeDtypeStruct((8, seqs, 1024), BF16)],
        scratch_shapes=[
            pltpu.VMEM((2, seqs * PAD, 128), F32),
            pltpu.VMEM((32, seqs, 256), BF16),
            pltpu.VMEM((1024, 128), F32),
            pltpu.VMEM((32 * PAD, 128), F32),
            pltpu.VMEM((4, seqs, 256), BF16),
        ],
        cost_estimate=pl.CostEstimate(flops=800_000_000, transcendentals=rows, bytes_accessed=4 * rows * 256),
        name="front",
    )(x, wf_t)
    return outs[:4], outs[4:8], outs[8]


def merge_left(pieces):
    seqs = pieces[0].shape[0] * 4

    def kernel(p0, p1, p2, p3, o_ref):
        x = jnp.concatenate([p0[...], p1[...], p2[...], p3[...]], axis=0).astype(F32)
        o_ref[...] = x.T.astype(BF16)

    vmem = pl.BlockSpec(memory_space=pltpu.VMEM)
    out = pl.pallas_call(
        kernel,
        in_specs=[vmem] * 4,
        out_shape=jax.ShapeDtypeStruct((256, seqs), BF16),
        cost_estimate=pl.CostEstimate(flops=100_000_000, transcendentals=0, bytes_accessed=4 * 256 * seqs),
        name="merge_left",
    )(*pieces)
    return out.reshape(8, 32, seqs)


def attend(items, wq, wg, wo):
    seqs = items[0][0].shape[0]
    ones = jnp.ones((16, items[0][1].shape[0]), BF16)
    scale = math.log2(math.e) / math.sqrt(HC)
    quads = HEADS // 4
    ready = []
    for mine, keys, v_t in items:
        q_t = dot(wq, mine, TT)
        q_t = jnp.concatenate([q_t, q_t], axis=1)
        first = lax.broadcasted_iota(jnp.int32, q_t.shape, 1) < seqs
        q_even = jnp.where(first, q_t, 0.0).astype(BF16)
        q_odd = jnp.where(first, 0.0, q_t).astype(BF16)
        ready.append((q_even, q_odd, jax.nn.sigmoid(dot(wg, mine, TT))))

    def spread(n, h):
        q_even, q_odd, _ = ready[n]
        parts = [q_even[h * HC:(h + 1) * HC], q_odd[(h + 1) * HC:(h + 2) * HC]]
        if h:
            parts.insert(0, jnp.zeros((h * HC, 2 * seqs), BF16))
        if h < HEADS - 2:
            parts.append(jnp.zeros(((HEADS - 2 - h) * HC, 2 * seqs), BF16))
        return jnp.concatenate(parts, axis=0)

    def scores_of(n, p):
        rhs = jnp.concatenate([spread(n, 4 * p), spread(n, 4 * p + 2)], axis=1)
        return dot(items[n][1], rhs, NN)

    order = [(n, p) for n in range(len(items)) for p in range(quads)]
    gated = [[] for _ in items]
    updates = []
    ahead = scores_of(*order[0])
    for at, (n, p) in enumerate(order):
        scores = ahead
        if at + 1 < len(order):
            ahead = scores_of(*order[at + 1])
        weights = jnp.exp2(scores * scale).astype(BF16)
        v_t, g_t = items[n][2], ready[n][2]
        tiles = []
        for u in range(3):
            h = 4 * p + u
            lhs = jnp.concatenate([v_t[h * HC:(h + 2) * HC], ones], axis=0)
            out = dot(lhs, weights[:, u * 256:(u + 1) * 256], NN)
            tiles.append(out[:2 * HC] / out[2 * HC:2 * HC + 1])
        lo, hi = slice(0, HC), slice(HC, 2 * HC)
        heads = (
            tiles[0][lo, :192],
            jnp.concatenate([tiles[0][hi, 192:], tiles[1][lo, :128]], axis=1),
            jnp.concatenate([tiles[1][hi, 128:], tiles[2][lo, :64]], axis=1),
            tiles[2][hi, 64:],
        )
        for u, att in enumerate(heads):
            h = 4 * p + u
            gated[n].append((g_t[h * HC:(h + 1) * HC] * att).astype(BF16))
        if p == quads - 1:
            updates.append(dot(jnp.concatenate(gated[n], axis=0), wo, TN))
    return updates


def finish(g, of, part, o_refs):
    @pl.when(g == pl.num_programs(0) - 1)
    def _():
        for k, o_ref in enumerate(o_refs):
            sl = slice(k * part * 8, (k + 1) * part * 8)
            o_ref[:, :128] = of[0, sl, :].astype(BF16)
            o_ref[:, 128:] = of[1, sl, :].astype(BF16)


def far_kernel(n_wait, *refs):
    x_refs, (wq_ref, wkv_ref, wg_ref, wo_ref) = refs[:4], refs[4:8]
    oa, ob, k_ref, v_ref, of = refs[8 + n_wait:]
    g = pl.program_id(0)
    at_once, part = x_refs[0].shape[:2]
    items = []
    for n in range(at_once):
        x = jnp.concatenate([b[n] for b in x_refs], axis=0)
        keys = dot(x, wkv_ref[:, :256], NN).astype(BF16)
        v_t = dot(wkv_ref[:, 256:], x, TT).astype(BF16)
        k_ref[n] = keys
        v_ref[n] = v_t
        items.append((x[2 * part:], keys, v_t))
    for n, update in enumerate(attend(items, wq_ref[...], wg_ref[...], wo_ref[...])):
        rows = pl.ds(g * at_once + n, 2 * part, stride=8)
        of[0, rows, :] = update[:, :128]
        of[1, rows, :] = update[:, 128:]
    finish(g, of, part, (oa, ob))


def near_kernel(n_wait, *refs):
    x_refs, (k_ref, v_ref), (wq_ref, wg_ref, wo_ref) = refs[:2], refs[2:4], refs[4:7]
    oa, ob, of = refs[7 + n_wait:]
    g = pl.program_id(0)
    at_once, part = x_refs[0].shape[:2]
    items = [
        (jnp.concatenate([b[n] for b in x_refs], axis=0), k_ref[n], v_ref[n]) for n in range(at_once)
    ]
    for n, update in enumerate(attend(items, wq_ref[...], wg_ref[...], wo_ref[...])):
        rows = pl.ds(g * at_once + n, 2 * part, stride=8)
        of[0, rows, :] = update[:, :128]
        of[1, rows, :] = update[:, 128:]
    finish(g, of, part, (oa, ob))


def attention(blocks, kept, weights, waits):
    count, part, width = blocks[0].shape
    seqs = 4 * part
    full = pl.BlockSpec((256, 256), lambda r: (0, 0))
    by_residue = lambda *tail: pl.BlockSpec((AT_ONCE, *tail), lambda r: (r, 0, 0))
    out_specs = [pl.BlockSpec((part * count, width), lambda r: (0, 0))] * 2
    out_shape = [jax.ShapeDtypeStruct((part * count, width), BF16)] * 2
    wq, wkv, wg, wo = weights
    if kept is None:
        kernel = far_kernel
        operands = (*blocks, wq, wkv, wg, wo)
        in_specs = [by_residue(part, width)] * 4 + [full, pl.BlockSpec((256, 512), lambda r: (0, 0)), full, full]
        out_specs += [by_residue(seqs, width), by_residue(width, seqs)]
        out_shape += [
            jax.ShapeDtypeStruct((count, seqs, width), BF16),
            jax.ShapeDtypeStruct((count, width, seqs), BF16),
        ]
    else:
        kernel = near_kernel
        operands = (*blocks[:2], *kept, wq, wg, wo)
        in_specs = [by_residue(part, width)] * 2 + [by_residue(seqs, width), by_residue(width, seqs)] + [full] * 3
    return pl.pallas_call(
        lambda *refs: kernel(len(waits), *refs),
        grid=(count // AT_ONCE,),
        in_specs=in_specs + after(*waits),
        out_specs=out_specs,
        out_shape=out_shape,
        scratch_shapes=[pltpu.VMEM((2, 2 * part * count, 128), F32)],
        cost_estimate=pl.CostEstimate(
            flops=count * (seqs * seqs * 256 * 9 + 2 * seqs * 256 * 256 * 4),
            transcendentals=count * HEADS * seqs * seqs // 2,
            bytes_accessed=4 * count * seqs * width,
        ),
    )(*operands, *waits)


def pair_kernel(scaling, r0, count, *refs):
    l_refs, right_refs, w_ref = refs[:8], refs[8:10], refs[10]
    o_ref, scr = refs[-2:]
    seqs = l_refs[0].shape[-1]
    rows = 8 * count
    xy = lax.axis_index(XY)
    left = jnp.concatenate([l[r0:r0 + count].reshape(count * 32, seqs) for l in l_refs], axis=0)
    for n in range(8):
        lanes = slice(n * 128, (n + 1) * 128)
        src = []
        for b in range(4):
            m = (b % 2) * 4 + (b // 2) * 2
            src.append(
                jnp.concatenate([x[xy ^ (m + h), :, lanes] for h in range(2) for x in right_refs], axis=0)
            )
        right = jnp.concatenate([x[:, e * 32:(e + 1) * 32] for e in range(4) for x in src], axis=1)
        o = dot(left, right, NN).astype(BF16)
        for i in range(rows):
            for e in range(4):
                row = (n * 4 + e) * 32
                scr[i, row:row + 32, :] = o[i * 32:(i + 1) * 32, e * 128:(e + 1) * 128]
    at = lax.axis_index(ROWS)
    for k in range(rows // 2):
        rhs = jnp.concatenate([scr[2 * k], scr[2 * k + 1]], axis=1)
        t = dot(w_ref[...], rhs, NN) * scaling
        for u in range(2):
            i = 2 * k + u
            o_ref[at ^ (i // count), i % count] = t[:, u * 128:(u + 1) * 128].T.astype(BF16)


def pair_block(left, rights, w_t, r0, count, scaling, waits):
    seqs = left[0].shape[-1]
    vmem = pl.BlockSpec(memory_space=pltpu.VMEM)
    return pl.pallas_call(
        lambda *refs: pair_kernel(scaling, r0, count, *refs),
        in_specs=[vmem] * 11 + after(*waits),
        out_specs=vmem,
        out_shape=jax.ShapeDtypeStruct((8, count, 128, 128), BF16),
        scratch_shapes=[pltpu.VMEM((8 * count, 1024, 128), BF16)],
        cost_estimate=pl.CostEstimate(
            flops=(2 * 256 * 4096 * seqs + 2 * 8 * 128 * 128 * 1024) * count,
            transcendentals=0,
            bytes_accessed=2 * (4096 + 512) * seqs,
        ),
    )(*left, *rights, w_t, *waits)


def place(blocks, wheres, shape, prior):
    n = len(blocks)
    more = [] if prior is None else [prior]

    def kernel(*refs):
        ins, out, sems = refs[:n], refs[-2], refs[-1]
        pairs = [p for b, where in zip(ins, wheres) for p in where(b, out)]
        copies = [pltpu.make_async_copy(a, to, sems.at[k]) for k, (a, to) in enumerate(pairs)]
        for c in copies:
            c.start()
        for c in copies:
            c.wait()

    hbm = pl.BlockSpec(memory_space=pltpu.HBM)
    return pl.pallas_call(
        kernel,
        in_specs=[pl.BlockSpec(memory_space=pltpu.VMEM)] * n + [hbm] * len(more),
        out_specs=hbm,
        out_shape=jax.ShapeDtypeStruct(shape, BF16),
        scratch_shapes=[pltpu.SemaphoreType.DMA((32,))],
        input_output_aliases={n: 0} if more else {},
        cost_estimate=pl.CostEstimate(flops=300_000_000, transcendentals=0, bytes_accessed=4_000_000),
    )(*blocks, *more)


def place_update(blocks):
    seqs, own, width = blocks[0].shape

    def to_group(k):
        return lambda b, out: [(b, out.at[:, lax.axis_index(SEQ) ^ k])]

    out = place(blocks, [to_group(k) for k in range(4)], (seqs, 4, own, width), None)
    return out.reshape(seqs, 4 * own, width)


def place_pair(got, prior, r0):
    count = got.shape[1]
    shape = (8, 4, 8, 32, 128)
    more = [] if prior is None else [prior]

    def kernel(g_hbm, *refs):
        out, buf, in_sems, out_sems = refs[-4:]
        loads = [pltpu.make_async_copy(g_hbm.at[k], buf.at[k], in_sems.at[k]) for k in range(8)]
        for c in loads:
            c.start()
        stores = []
        for k in range(8):
            loads[k].wait()
            for b in range(4):
                v = lax.axis_index(("yh", "xl")) ^ b
                a = (v % 2) * 2 + v // 2
                to = out.at[pl.ds(r0, count), a, k]
                stores.append(pltpu.make_async_copy(buf.at[k, :, b], to, out_sems.at[4 * k + b]))
                stores[-1].start()
        for c in stores:
            c.wait()

    hbm = pl.BlockSpec(memory_space=pltpu.HBM)
    return pl.pallas_call(
        kernel,
        in_specs=[hbm] * (1 + len(more)),
        out_specs=hbm,
        out_shape=jax.ShapeDtypeStruct(shape, BF16),
        scratch_shapes=[
            pltpu.VMEM((8, count, 4, 32, 128), BF16),
            pltpu.SemaphoreType.DMA((8,)),
            pltpu.SemaphoreType.DMA((32,)),
        ],
        input_output_aliases={1: 0} if more else {},
        cost_estimate=pl.CostEstimate(flops=300_000_000, transcendentals=0, bytes_accessed=4_000_000),
    )(pltpu.with_memory_space_constraint(got.reshape(8, count, 4, 32, 128), pltpu.HBM), *more)


def swap(x, axes, k):
    n = lax.axis_size(axes)
    return lax.ppermute(x, axes, [(j, j ^ k) for j in range(n)])


def layer(alignment, query_weight, w_keyval, w_gate, output_weight, w_factors, w_pair_out):
    seqs, residues, width = alignment.shape
    own = residues // 4
    total = seqs * 4
    normed, lefts, right = front(alignment.reshape(seqs * residues, width), w_factors.T)
    blocks = [normed[0]] + [swap(normed[k], SEQ, k) for k in (1, 2, 3)]
    near = lax.all_to_all(right, XY, 0, 0)
    pieces = [lefts[0]] + [swap(lefts[k], SEQ, k) for k in (1, 2, 3)]
    left = merge_left(pieces)
    left_y = swap(left, ROWS, 4)
    left8 = [left] + [swap(left, ROWS, k) for k in (1, 2, 3)]
    left8 += [left_y] + [swap(left_y, ROWS, k) for k in (1, 2, 3)]
    rights = [near, swap(near, ("c",), 1)]

    w_pair_out, left = lax.optimization_barrier((w_pair_out, left))
    weights = (query_weight, w_keyval, w_gate, output_weight)
    w_t = w_pair_out.reshape(32, 32, 128).transpose(2, 1, 0).reshape(128, 1024)
    scaling = 1.0 / total
    u2, u3, *kept = attention(blocks, None, weights, (left_y, w_t))
    backs = [None, None, swap(u2, SEQ, 2), swap(u3, SEQ, 3)]
    out0 = pair_block(left8, rights, w_t, 0, SPLIT, scaling, (u2,))
    got0 = lax.all_to_all(out0, ROWS, 0, 0)
    out1 = pair_block(left8, rights, w_t, SPLIT, 8 - SPLIT, scaling, (out0,))
    got1 = lax.all_to_all(out1, ROWS, 0, 0)
    pair = place_pair(got0, None, 0)
    u0, u1 = attention(blocks, kept, weights, (out1, pair))
    backs[0], backs[1] = u0, swap(u1, SEQ, 1)
    alignment_update = place_update([b.reshape(seqs, own, width) for b in backs])
    pair = place_pair(got1, pair, SPLIT)
    return alignment_update, pair.reshape(8, 1024, 128)


def solution(mesh):
    split = Mesh(
        mesh.devices.reshape(2, 2, 2, 4, 2, 2), ("xl", "yh", "yl", "z", "xh", "c")
    )
    res = ("xl", "yh", "yl", "z")
    in_specs = (P(SEQ, res, None), P(), P(), P(), P(), P(), P())
    out_specs = (P(SEQ, res, None), P((*res, *SEQ), None, None))
    return jax.shard_map(layer, mesh=split, in_specs=in_specs, out_specs=out_specs, check_vma=False)
```
